32 devices in a mesh: dp: 4 (over x, core), tensor: 8 (over z, y).
Axes of the slice: x: 2, y: 2, z: 4, core: 2. Of those that a mesh axis runs over, the one named last changes fastest.
Arguments:
- activations: bfloat16 [1024, 5120], P('dp'), may hold values from -6 to 6
- grad_out: bfloat16 [1024, 5120], P('dp'), may hold values from -6 to 6
- gate_pre: bfloat16 [1024, 7168], P('dp', 'tensor'), may hold values from -8 to 8
- up_pre: bfloat16 [1024, 7168], P('dp', 'tensor'), may hold values from -6 to 6
- gate_up: bfloat16 [5120, 2, 7168], P('dp', None, 'tensor'), may hold values from -0.078125 to 0.078125
- down_weight: bfloat16 [5120, 7168], P('dp', 'tensor'), may hold values from -0.0625 to 0.0625
Outputs:
- grad_input: bfloat16 [1024, 5120], P('dp')
- grad_gate_up: float32 [5120, 2, 7168], P('dp', None, 'tensor')
- grad_down: float32 [5120, 7168], P('dp', 'tensor')
The draws below stay inside these ranges and needn't reach their ends.
All inputs are finite; a program needn't handle non-finite values.
Results may differ from the reference program's by a relative error of at most 0.017.
Values may be sent and summed in bfloat16 or wider, within the bound.
A program may use at most 128 MiB of HBM per device.

```python
import jax
import jax.numpy as jnp
from jax import lax

D = 5120
FF = 7168
TOK_DEV = 256
TOKENS = 1024
N_DP = 4
N_TENSOR = 8


def raised(result, stream_key, source, target, blocks, factor):
    owner, partner = [(jnp.arange(result.shape[dim]) // (result.shape[dim] // blocks)).reshape([-1 if axis == dim else 1 for axis in range(result.ndim)]) for dim in (source, target)]
    chosen = jax.random.permutation(stream_key, blocks)[partner]
    strong = (owner == chosen) | (owner == (partner + blocks // 2) % blocks)
    return jnp.where(strong, factor * result, result)


def shard_levels(own_key, extent, cuts, low, high):
    def one(dim, shards_of):
        draws = jax.random.uniform(jax.random.fold_in(jax.random.fold_in(own_key, 6), dim), (shards_of,), jnp.float32, low / len(cuts), high / len(cuts))
        return jnp.repeat(jnp.exp(draws), extent[dim] // shards_of).reshape((-1,) + (1,) * (len(extent) - dim - 1))

    gain = one(*cuts[0])
    for cut in cuts[1:]:
        gain = gain * one(*cut)
    return gain


def scatter_about(own_key, dims, scale, bound, shards=(), kind=jnp.bfloat16):
    array = jax.random.normal(own_key, dims, jnp.float32) * scale
    if len(shards) > 0:
        array = shard_levels(own_key, dims, shards, -0.22, 0.18) * array
    return jnp.clip(array, min=-bound, max=bound).astype(kind)


def gaussian_with(key, shape, scale, bound, split, heavy, kind=jnp.bfloat16):
    drawn = scale * jax.random.normal(key, shape, jnp.float32)
    if split:
        drawn = drawn * shard_levels(key, shape, split, -0.22, 0.18)
    return jnp.clip(raised(drawn, jax.random.fold_in(key, 3), *heavy), -bound, bound).astype(kind)


def setup_inputs(seed: int = 0) -> dict:
    key_list = jax.random.split(jax.random.key(seed), 7)
    return {
        "activations": gaussian_with(key_list[0], (TOKENS, D), 1.0, 6.0, ((0, 4),), (0, 1, 4, 2.0)),
        "grad_out": gaussian_with(key_list[1], (TOKENS, D), 1.0, 6.0, ((0, 4),), (0, 1, 4, 2.0)),
        "gate_pre": scatter_about(key_list[2], (TOKENS, FF), 1.5, 8.0, ((0, 4), (1, 8))),
        "up_pre": scatter_about(key_list[3], (TOKENS, FF), 1.0, 6.0, ((0, 4), (1, 8))),
        "gate_up": scatter_about(key_list[4], (D, 2, FF), D ** -0.5, 0.078125, ((0, 4), (2, 8))),
        "down_weight": scatter_about(key_list[5], (D, FF), FF ** -0.5, 0.0625, ((0, 4), (1, 8))),
    }


def reference(activations, grad_out, gate_pre, up_pre, gate_up, down_weight):
    gate_wide = gate_pre.astype(jnp.float32)
    up_wide = up_pre.astype(jnp.float32)
    gate_sigmoid = jax.nn.sigmoid(gate_wide)
    gate_silu = gate_wide * gate_sigmoid
    hidden = (gate_silu * up_wide).astype(jnp.bfloat16)
    grad_h = jnp.dot(grad_out, down_weight, preferred_element_type=jnp.float32)
    grad_gate = grad_h * up_wide * gate_sigmoid * (1.0 + gate_wide * (1.0 - gate_sigmoid))
    grad_up = grad_h * gate_silu
    grad_hidden = jnp.stack([grad_gate, grad_up], axis=1).astype(jnp.bfloat16)

    group_width = FF // N_TENSOR
    hidden_groups = grad_hidden.reshape(TOKENS, 2, N_TENSOR, group_width).transpose(2, 0, 1, 3)
    hidden_groups = hidden_groups.reshape(N_TENSOR, TOKENS, 2 * group_width)
    weight_groups = gate_up.reshape(D, 2, N_TENSOR, group_width).transpose(2, 0, 1, 3)
    weight_groups = weight_groups.reshape(N_TENSOR, D, 2 * group_width)

    def add_part(running, paired):
        left_rows, right_rows = paired
        part_sum = jnp.dot(left_rows, right_rows.T, preferred_element_type=jnp.float32)
        part_sum = lax.optimization_barrier(part_sum.astype(jnp.bfloat16))
        return running + part_sum.astype(jnp.float32), None

    input_total, _ = lax.scan(add_part, jnp.zeros((TOKENS, D), jnp.float32), (hidden_groups, weight_groups))
    grad_input = input_total.astype(jnp.bfloat16)

    act_groups = activations.reshape(N_DP, TOK_DEV, D)
    out_groups = grad_out.reshape(N_DP, TOK_DEV, D)
    grad_groups = grad_hidden.reshape(N_DP, TOK_DEV, 2 * FF)
    plain_groups = hidden.reshape(N_DP, TOK_DEV, FF)

    def add_group(running, group_items):
        act_rows, out_rows, grad_rows, plain_rows = group_items
        gate_part = jnp.dot(act_rows.T, grad_rows, preferred_element_type=jnp.float32)
        down_part = jnp.dot(out_rows.T, plain_rows, preferred_element_type=jnp.float32)
        gate_part = lax.optimization_barrier(gate_part.astype(jnp.bfloat16))
        down_part = lax.optimization_barrier(down_part.astype(jnp.bfloat16))
        return (running[0] + gate_part.astype(jnp.float32), running[1] + down_part.astype(jnp.float32)), None

    start_sums = (jnp.zeros((D, 2 * FF), jnp.float32), jnp.zeros((D, FF), jnp.float32))
    summed, _ = lax.scan(add_group, start_sums, (act_groups, out_groups, grad_groups, plain_groups))
    grad_gate_up = (summed[0] / N_DP).reshape(D, 2, FF)
    grad_down = summed[1] / N_DP
    return grad_input, grad_gate_up, grad_down
```

```python
import jax
import jax.numpy as jnp
from jax import lax
from jax.experimental import pallas as pl
from jax.experimental.pallas import tpu as pltpu
from jax.sharding import PartitionSpec as P

MESH = pl.DeviceIdType.MESH
ANY = pl.BlockSpec(memory_space=pl.ANY)
VMEM = pl.BlockSpec(memory_space=pltpu.VMEM)


def remote(src, dst, send, recv, device):
    return pltpu.make_async_remote_copy(
        src_ref=src, dst_ref=dst, send_sem=send, recv_sem=recv, device_id=device, device_id_type=MESH
    )


def greet(axes):
    barrier = pltpu.get_barrier_semaphore()
    count = 0
    for axis in axes:
        n = lax.axis_size(axis)
        me = lax.axis_index(axis)
        for s in range(1, n):
            pl.semaphore_signal(
                barrier, inc=1, device_id={axis: lax.rem(me + s, n)}, device_id_type=MESH
            )
        count += n - 1
    pl.semaphore_wait(barrier, count)


def spread(cid, block, wide=()):
    n = lax.axis_size("dp")
    m = lax.axis_size("tensor")
    w = len(wide)
    rows, width = block.shape[1:]

    def kernel(*refs):
        block_ref = refs[0]
        wide_refs = refs[1 : 1 + w]
        out_ref = refs[1 + w]
        wide_outs = refs[2 + w : 2 + 2 * w]
        s1, r1, s2, r2, sw, rw, local = refs[2 + 2 * w :]
        me = lax.axis_index("dp")
        j = lax.axis_index("tensor")
        partner = me + 1 - 2 * lax.rem(me, 2)
        greet(("dp", "tensor"))
        sends = []
        for s in range(1, n):
            p = lax.rem(me + s, n)
            sends.append(
                remote(block_ref.at[p], out_ref.at[me, j], s1.at[s], r1.at[me], {"dp": p})
            )
            sends[-1].start()
        locals_ = [pltpu.make_async_copy(block_ref.at[me], out_ref.at[me, j], local.at[w])]
        locals_[-1].start()
        for a in range(w):
            for s in range(1, n // 2):
                q = lax.rem(me + 2 * s, n)
                sends.append(
                    remote(wide_refs[a], wide_outs[a].at[me], sw.at[a, s], rw.at[a, me], {"dp": q})
                )
                sends[-1].start()
        for a in range(w):
            sends.append(
                remote(wide_refs[a], wide_outs[a].at[me], sw.at[a, 0], rw.at[a, me], {"dp": partner})
            )
            sends[-1].start()
            locals_.append(pltpu.make_async_copy(wide_refs[a], wide_outs[a].at[me], local.at[a]))
            locals_[-1].start()
        for s in range(1, n):
            p = lax.rem(me + n - s, n)
            remote(block_ref.at[p], out_ref.at[p, j], s1.at[s], r1.at[p], {"dp": p}).wait_recv()
        locals_[0].wait()
        for s in range(1, m):
            k = lax.rem(j + s, m)
            sends.append(
                remote(out_ref.at[:, j], out_ref.at[:, j], s2.at[s], r2.at[j], {"tensor": k})
            )
            sends[-1].start()
        for a in range(w):
            for s in range(1, n // 2):
                q = lax.rem(me + n - 2 * s, n)
                remote(
                    wide_refs[a], wide_outs[a].at[q], sw.at[a, s], rw.at[a, q], {"dp": q}
                ).wait_recv()
                sends.append(
                    remote(
                        wide_outs[a].at[q],
                        wide_outs[a].at[q],
                        sw.at[a, n // 2 + s - 1],
                        rw.at[a, q],
                        {"dp": partner},
                    )
                )
                sends[-1].start()
        for a in range(w):
            locals_[1 + a].wait()
            for s in range(n // 2):
                q = lax.rem(partner + 2 * s, n)
                remote(
                    wide_refs[a], wide_outs[a].at[q], sw.at[a, s], rw.at[a, q], {"dp": partner}
                ).wait_recv()
        for s in range(1, m):
            k = lax.rem(j + m - s, m)
            remote(
                out_ref.at[:, k], out_ref.at[:, k], s2.at[s], r2.at[k], {"tensor": k}
            ).wait_recv()
        for copy in sends:
            copy.wait_send()

    dma = pltpu.SemaphoreType.DMA
    shapes = [jax.ShapeDtypeStruct((n, m, rows, width), block.dtype)]
    shapes += [jax.ShapeDtypeStruct((n,) + a.shape, a.dtype) for a in wide]
    return pl.pallas_call(
        kernel,
        out_shape=shapes,
        in_specs=[VMEM] * (1 + w),
        out_specs=[ANY] * (1 + w),
        scratch_shapes=[
            dma((n,)),
            dma((n,)),
            dma((m,)),
            dma((m,)),
            dma((max(w, 1), n)),
            dma((max(w, 1), n)),
            dma((w + 1,)),
        ],
        compiler_params=pltpu.CompilerParams(collective_id=cid, has_side_effects=True),
    )(block, *wide)


def trade(cid, parts):
    n, m, rows, width = parts.shape

    def kernel(src, dst, send, recv, local):
        j = lax.axis_index("tensor")
        greet(("tensor",))
        sends = []
        for s in range(1, m):
            k = lax.rem(j + s, m)
            sends.append(remote(src.at[:, k], dst.at[j], send.at[s], recv.at[j], {"tensor": k}))
            sends[-1].start()
        own = pltpu.make_async_copy(src.at[:, j], dst.at[j], local)
        own.start()
        for s in range(1, m):
            k = lax.rem(j + m - s, m)
            remote(src.at[:, k], dst.at[k], send.at[s], recv.at[k], {"tensor": k}).wait_recv()
        own.wait()
        for copy in sends:
            copy.wait_send()

    dma = pltpu.SemaphoreType.DMA
    return pl.pallas_call(
        kernel,
        out_shape=jax.ShapeDtypeStruct((m, n, rows, width), parts.dtype),
        in_specs=[ANY],
        out_specs=ANY,
        scratch_shapes=[dma((m,)), dma((m,)), dma],
        compiler_params=pltpu.CompilerParams(collective_id=cid, has_side_effects=True),
    )(parts)


def add_over_dp(partial):
    n = partial.shape[0]
    me = lax.axis_index("dp")
    core = lax.rem(me, 2)
    pairs = partial.reshape((n // 2, 2) + partial.shape[1:])
    other = lax.dynamic_index_in_dim(pairs, 1 - core, 1, keepdims=False).astype(jnp.bfloat16)
    keep = lax.dynamic_index_in_dim(pairs, core, 1, keepdims=False)
    came = lax.ppermute(other, "dp", [(i, i ^ 1) for i in range(n)])
    half = keep + came.astype(jnp.float32)
    mine = me // 2
    total = lax.dynamic_index_in_dim(half, mine, 0, keepdims=False)
    for s in range(1, n // 2):
        piece = lax.dynamic_index_in_dim(half, lax.rem(mine + s, n // 2), 0, keepdims=False)
        came = lax.ppermute(
            piece.astype(jnp.bfloat16), "dp", [(i, (i + 2 * s) % n) for i in range(n)]
        )
        total = total + came.astype(jnp.float32)
    return total.astype(jnp.bfloat16)


def per_device(activations, grad_out, gate_pre, up_pre, gate_up, down_weight):
    tokens, model = activations.shape
    slab, hidden_width = down_weight.shape
    n = lax.axis_size("dp")
    m = lax.axis_size("tensor")
    rows = tokens // m
    j = lax.axis_index("tensor")

    def own_rows(a):
        piece = lax.dynamic_slice_in_dim(a, j * rows, rows, 0)
        return piece.reshape(rows, n, slab).transpose(1, 0, 2)

    dy, gate_all, up_all = spread(1, own_rows(grad_out), (gate_pre, up_pre))
    dy_cols = dy.reshape(n * tokens, slab)
    partial = jnp.dot(dy_cols, down_weight, preferred_element_type=jnp.float32)
    grad_h = add_over_dp(partial.reshape(n, tokens, hidden_width))
    x, grad_h_all = spread(2, own_rows(activations), (grad_h,))
    x_cols = x.reshape(n * tokens, slab)

    def flat(a):
        return a.reshape(n * tokens, hidden_width).astype(jnp.float32)

    gate_wide, up_wide, grad_h = flat(gate_all), flat(up_all), flat(grad_h_all)
    gate_sigmoid = jax.nn.sigmoid(gate_wide)
    gate_silu = gate_wide * gate_sigmoid
    hidden = (gate_silu * up_wide).astype(jnp.bfloat16)
    grad_gate = grad_h * up_wide * gate_sigmoid * (1.0 + gate_wide * (1.0 - gate_sigmoid))
    grad_gate = grad_gate.astype(jnp.bfloat16)
    grad_up = (grad_h * gate_silu).astype(jnp.bfloat16)
    grad_hidden = jnp.concatenate([grad_gate, grad_up], axis=1)

    part = lax.dot_general(
        grad_hidden,
        gate_up.reshape(slab, 2 * hidden_width),
        (((1,), (1,)), ((), ())),
        preferred_element_type=jnp.float32,
    ).astype(jnp.bfloat16)
    parts = trade(3, part.reshape(n, m, rows, slab))
    summed = jnp.sum(parts.astype(jnp.float32), axis=0).astype(jnp.bfloat16)
    (gathered,) = spread(4, summed)
    grad_input = gathered.transpose(1, 2, 0, 3).reshape(tokens, model)

    def weight(a, b):
        total = lax.dot_general(
            a, b, (((0,), (0,)), ((), ())), preferred_element_type=jnp.float32
        )
        return total / n

    grad_gate_up = jnp.stack([weight(x_cols, grad_gate), weight(x_cols, grad_up)], axis=1)
    grad_down = weight(dy_cols, hidden)
    return (grad_input, grad_gate_up, grad_down)


def solution(mesh):
    in_specs = (
        P("dp", None),
        P("dp", None),
        P("dp", "tensor"),
        P("dp", "tensor"),
        P("dp", None, "tensor"),
        P("dp", "tensor"),
    )
    out_specs = (P("dp", None), P("dp", None, "tensor"), P("dp", "tensor"))
    return jax.shard_map(
        per_device, mesh=mesh, in_specs=in_specs, out_specs=out_specs, check_vma=False
    )
```

```python
import jax
import jax.numpy as jnp
from jax import lax
from jax.experimental import pallas as pl
from jax.experimental.pallas import tpu as pltpu
from jax.sharding import PartitionSpec as P

MESH = pl.DeviceIdType.MESH
ANY = pl.BlockSpec(memory_space=pl.ANY)
VMEM = pl.BlockSpec(memory_space=pltpu.VMEM)


def remote(src, dst, send, recv, device):
    return pltpu.make_async_remote_copy(
        src_ref=src, dst_ref=dst, send_sem=send, recv_sem=recv, device_id=device, device_id_type=MESH
    )


def greet(axes):
    barrier = pltpu.get_barrier_semaphore()
    count = 0
    for axis in axes:
        n = lax.axis_size(axis)
        me = lax.axis_index(axis)
        for s in range(1, n):
            pl.semaphore_signal(
                barrier, inc=1, device_id={axis: lax.rem(me + s, n)}, device_id_type=MESH
            )
        count += n - 1
    pl.semaphore_wait(barrier, count)


def spread(cid, block, wide=()):
    n = lax.axis_size("dp")
    m = lax.axis_size("tensor")
    w = len(wide)
    rows, width = block.shape[1:]

    def kernel(*refs):
        block_ref = refs[0]
        wide_refs = refs[1 : 1 + w]
        out_ref = refs[1 + w]
        wide_outs = refs[2 + w : 2 + 2 * w]
        s1, r1, s2, r2, sw, rw, local = refs[2 + 2 * w :]
        me = lax.axis_index("dp")
        j = lax.axis_index("tensor")
        partner = me + 1 - 2 * lax.rem(me, 2)
        greet(("dp", "tensor"))
        sends = []
        for s in range(1, n):
            p = lax.rem(me + s, n)
            sends.append(
                remote(block_ref.at[p], out_ref.at[me, j], s1.at[s], r1.at[me], {"dp": p})
            )
            sends[-1].start()
        locals_ = [pltpu.make_async_copy(block_ref.at[me], out_ref.at[me, j], local.at[w])]
        locals_[-1].start()
        for a in range(w):
            for s in range(1, n // 2):
                q = lax.rem(me + 2 * s, n)
                sends.append(
                    remote(wide_refs[a], wide_outs[a].at[me], sw.at[a, s], rw.at[a, me], {"dp": q})
                )
                sends[-1].start()
        for a in range(w):
            sends.append(
                remote(wide_refs[a], wide_outs[a].at[me], sw.at[a, 0], rw.at[a, me], {"dp": partner})
            )
            sends[-1].start()
            locals_.append(pltpu.make_async_copy(wide_refs[a], wide_outs[a].at[me], local.at[a]))
            locals_[-1].start()
        for s in range(1, n):
            p = lax.rem(me + n - s, n)
            remote(block_ref.at[p], out_ref.at[p, j], s1.at[s], r1.at[p], {"dp": p}).wait_recv()
        locals_[0].wait()
        lines = m // 2
        row, column = j // 2, lax.rem(j, 2)
        facing = j + 1 - 2 * column
        first, last = row == 0, row == lines - 1

        def hop(kind, r, device):
            k = 2 * r + column
            return remote(
                out_ref.at[:, k], out_ref.at[:, k], s2.at[kind, r], r2.at[k], {"tensor": device}
            )

        def up(r):
            return hop(0, r, lax.rem(j + 2, m))

        def down(r):
            return hop(1, r, lax.rem(j + m - 2, m))

        def across(r):
            return hop(2, r, facing)

        for d in range(lines):
            below, above = row - d, row + d

            @pl.when(below >= 0)
            def _():
                if d > 0:
                    up(below).wait_recv()
                pl.when(jnp.logical_not(last))(lambda: up(below).start())
                if d == 0:
                    pl.when(jnp.logical_not(first))(lambda: down(row).start())
                across(below).start()

            if d > 0:

                @pl.when(above < lines)
                def _():
                    down(above).wait_recv()
                    pl.when(jnp.logical_not(first))(lambda: down(above).start())
                    across(above).start()

        for a in range(w):
            for s in range(1, n // 2):
                q = lax.rem(me + n - 2 * s, n)
                remote(
                    wide_refs[a], wide_outs[a].at[q], sw.at[a, s], rw.at[a, q], {"dp": q}
                ).wait_recv()
                sends.append(
                    remote(
                        wide_outs[a].at[q],
                        wide_outs[a].at[q],
                        sw.at[a, n // 2 + s - 1],
                        rw.at[a, q],
                        {"dp": partner},
                    )
                )
                sends[-1].start()
        for a in range(w):
            locals_[1 + a].wait()
            for s in range(n // 2):
                q = lax.rem(partner + 2 * s, n)
                remote(
                    wide_refs[a], wide_outs[a].at[q], sw.at[a, s], rw.at[a, q], {"dp": partner}
                ).wait_recv()
        for r in range(lines):
            k = 2 * r + 1 - column
            remote(
                out_ref.at[:, k], out_ref.at[:, k], s2.at[2, r], r2.at[k], {"tensor": facing}
            ).wait_recv()
            across(r).wait_send()
            went_up = jnp.logical_and(jnp.logical_not(last), r <= row)
            went_down = jnp.logical_and(jnp.logical_not(first), r >= row)
            pl.when(went_up)(lambda: up(r).wait_send())
            pl.when(went_down)(lambda: down(r).wait_send())
        for copy in sends:
            copy.wait_send()

    dma = pltpu.SemaphoreType.DMA
    shapes = [jax.ShapeDtypeStruct((n, m, rows, width), block.dtype)]
    shapes += [jax.ShapeDtypeStruct((n,) + a.shape, a.dtype) for a in wide]
    return pl.pallas_call(
        kernel,
        out_shape=shapes,
        in_specs=[VMEM] * (1 + w),
        out_specs=[ANY] * (1 + w),
        scratch_shapes=[
            dma((n,)),
            dma((n,)),
            dma((3, m // 2)),
            dma((m,)),
            dma((max(w, 1), n)),
            dma((max(w, 1), n)),
            dma((w + 1,)),
        ],
        compiler_params=pltpu.CompilerParams(collective_id=cid, has_side_effects=True),
    )(block, *wide)


def trade(cid, parts):
    n, m, rows, width = parts.shape

    def kernel(src, dst, send, recv, local):
        j = lax.axis_index("tensor")
        greet(("tensor",))
        sends = []
        for s in range(1, m):
            k = lax.rem(j + s, m)
            sends.append(remote(src.at[:, k], dst.at[j], send.at[s], recv.at[j], {"tensor": k}))
            sends[-1].start()
        own = pltpu.make_async_copy(src.at[:, j], dst.at[j], local)
        own.start()
        for s in range(1, m):
            k = lax.rem(j + m - s, m)
            remote(src.at[:, k], dst.at[k], send.at[s], recv.at[k], {"tensor": k}).wait_recv()
        own.wait()
        for copy in sends:
            copy.wait_send()

    dma = pltpu.SemaphoreType.DMA
    return pl.pallas_call(
        kernel,
        out_shape=jax.ShapeDtypeStruct((m, n, rows, width), parts.dtype),
        in_specs=[ANY],
        out_specs=ANY,
        scratch_shapes=[dma((m,)), dma((m,)), dma],
        compiler_params=pltpu.CompilerParams(collective_id=cid, has_side_effects=True),
    )(parts)


def add_over_dp(partial):
    n = partial.shape[0]
    me = lax.axis_index("dp")
    core = lax.rem(me, 2)
    pairs = partial.reshape((n // 2, 2) + partial.shape[1:])
    other = lax.dynamic_index_in_dim(pairs, 1 - core, 1, keepdims=False).astype(jnp.bfloat16)
    keep = lax.dynamic_index_in_dim(pairs, core, 1, keepdims=False)
    came = lax.ppermute(other, "dp", [(i, i ^ 1) for i in range(n)])
    half = keep + came.astype(jnp.float32)
    mine = me // 2
    total = lax.dynamic_index_in_dim(half, mine, 0, keepdims=False)
    for s in range(1, n // 2):
        piece = lax.dynamic_index_in_dim(half, lax.rem(mine + s, n // 2), 0, keepdims=False)
        came = lax.ppermute(
            piece.astype(jnp.bfloat16), "dp", [(i, (i + 2 * s) % n) for i in range(n)]
        )
        total = total + came.astype(jnp.float32)
    return total.astype(jnp.bfloat16)


def paired_weight(x_cols, grad_gate, grad_up, scale):
    depth, slab = x_cols.shape
    width = grad_gate.shape[1]
    tile = 128 if slab % 128 == 0 else slab

    def kernel(x_ref, gate_ref, up_ref, out_ref):
        for i, ref in enumerate((gate_ref, up_ref)):
            total = lax.dot_general(
                x_ref[...], ref[...], (((0,), (0,)), ((), ())), preferred_element_type=jnp.float32
            )
            out_ref[:, i, :] = total / scale

    whole = pl.BlockSpec((depth, width), lambda i: (0, 0))
    return pl.pallas_call(
        kernel,
        grid=(slab // tile,),
        out_shape=jax.ShapeDtypeStruct((slab, 2, width), jnp.float32),
        in_specs=[pl.BlockSpec((depth, tile), lambda i: (0, i)), whole, whole],
        out_specs=pl.BlockSpec((tile, 2, width), lambda i: (i, 0, 0)),
        cost_estimate=pl.CostEstimate(
            flops=4 * depth * slab * width, bytes_accessed=8 * slab * width, transcendentals=0
        ),
    )(x_cols, grad_gate, grad_up)


def per_device(activations, grad_out, gate_pre, up_pre, gate_up, down_weight):
    tokens, model = activations.shape
    slab, hidden_width = down_weight.shape
    n = lax.axis_size("dp")
    m = lax.axis_size("tensor")
    rows = tokens // m
    j = lax.axis_index("tensor")

    def own_rows(a):
        piece = lax.dynamic_slice_in_dim(a, j * rows, rows, 0)
        return piece.reshape(rows, n, slab).transpose(1, 0, 2)

    dy, gate_all, up_all = spread(1, own_rows(grad_out), (gate_pre, up_pre))
    dy_cols = dy.reshape(n * tokens, slab)
    partial = jnp.dot(dy_cols, down_weight, preferred_element_type=jnp.float32)
    grad_h = add_over_dp(partial.reshape(n, tokens, hidden_width))
    x, grad_h_all = spread(2, own_rows(activations), (grad_h,))
    x_cols = x.reshape(n * tokens, slab)

    def flat(a):
        return a.reshape(n * tokens, hidden_width).astype(jnp.float32)

    gate_wide, up_wide, grad_h = flat(gate_all), flat(up_all), flat(grad_h_all)
    gate_sigmoid = jax.nn.sigmoid(gate_wide)
    gate_silu = gate_wide * gate_sigmoid
    hidden = (gate_silu * up_wide).astype(jnp.bfloat16)
    grad_gate = grad_h * up_wide * gate_sigmoid * (1.0 + gate_wide * (1.0 - gate_sigmoid))
    grad_gate = grad_gate.astype(jnp.bfloat16)
    grad_up = (grad_h * gate_silu).astype(jnp.bfloat16)
    grad_hidden = jnp.concatenate([grad_gate, grad_up], axis=1)

    part = lax.dot_general(
        grad_hidden,
        gate_up.reshape(slab, 2 * hidden_width),
        (((1,), (1,)), ((), ())),
        preferred_element_type=jnp.float32,
    ).astype(jnp.bfloat16)
    parts = trade(3, part.reshape(n, m, rows, slab))
    summed = jnp.sum(parts.astype(jnp.float32), axis=0).astype(jnp.bfloat16)
    (gathered,) = spread(4, summed)
    grad_input = gathered.transpose(1, 2, 0, 3).reshape(tokens, model)

    def weight(a, b):
        total = lax.dot_general(
            a, b, (((0,), (0,)), ((), ())), preferred_element_type=jnp.float32
        )
        return total / n

    grad_gate_up = paired_weight(x_cols, grad_gate, grad_up, float(n))
    grad_down = weight(dy_cols, hidden)
    return (grad_input, grad_gate_up, grad_down)


def solution(mesh):
    in_specs = (
        P("dp", None),
        P("dp", None),
        P("dp", "tensor"),
        P("dp", "tensor"),
        P("dp", None, "tensor"),
        P("dp", "tensor"),
    )
    out_specs = (P("dp", None), P("dp", None, "tensor"), P("dp", "tensor"))
    return jax.shard_map(
        per_device, mesh=mesh, in_specs=in_specs, out_specs=out_specs, check_vma=False
    )
```
